128 devices in a mesh: prow: 8 (over z_hi, y), pcol: 16 (over x, z_lo, core).
Axes of the slice: x: 4, y: 4, z: 4 (z_hi: 2, z_lo: 2; z = z_hi * 2 + z_lo), core: 2. Of those that a mesh axis runs over, the one named last changes fastest.
Arguments:
- panel_t: float32 [16, 256, 8192], P('pcol', None, 'prow'), may hold values from -0.0625 to 0.0625
- ancestor: float32 [8192, 8192], P('prow', 'pcol'), as said below
- structure: int32 [16, 32], replicated, may hold values 0 or 1
- diag_inv: float32 [16, 256, 256], P('pcol'), may hold values from -6 to 6
Outputs:
- inverse_panel: float32 [4096, 8192], P('pcol', 'prow')
- inverse_diag: float32 [16, 256, 256], P('pcol')
The draws below stay inside these ranges and needn't reach their ends.
Inputs may be any that keep to these rules, and one draw needn't show every extreme that they name: ancestor is symmetric up to rounding.
All inputs are finite; a program needn't handle non-finite values.
Results may differ from the reference program's by a relative error of at most 0.00007.
Values sent between devices are 32-bit elements; how exact they have to be, the bound alone decides.
A program may use at most 128 MiB of HBM per device.

```python
import jax
import jax.numpy as jnp
from jax import lax

B = 256
S = 16
NA = 32
R = 8192


def draw_ancestor(key, part):
    first = jax.random.normal(jax.random.fold_in(key, 11), (R, R), jnp.float32)
    matrix = (first + first.T) * 0.7071
    return matrix


def place_ends(array, key, smallest, high):
    longest = array.shape.index(max(array.shape))
    spots = []
    for shift in (0, 1):
        where = [jax.random.randint(jax.random.fold_in(key, axis), (), 0, length) for axis, length in enumerate(array.shape)]
        where[longest] = (where[longest] + shift) % array.shape[longest]
        spots.append(tuple(where))
    return array.at[spots[0]].set(smallest).at[spots[1]].set(high)


def level_of(own_key, dims, split, smallest, top_value):
    def one(axis_at, parts):
        steps = jax.random.uniform(jax.random.fold_in(jax.random.fold_in(own_key, 6), axis_at), (parts,), jnp.float32, smallest / len(split), top_value / len(split))
        return jnp.repeat(jnp.exp(steps), dims[axis_at] // parts).reshape((-1,) + (1,) * (len(dims) - axis_at - 1))

    factor_of = one(*split[0])
    for cut in split[1:]:
        factor_of = factor_of * one(*cut)
    return factor_of


def gaussian(own_key, extent, spread, reach, split=(), held_as=jnp.bfloat16):
    values = jax.random.normal(own_key, extent, jnp.float32) * spread
    if len(split) > 0:
        values = level_of(own_key, extent, split, -0.22, 0.18) * values
    return jnp.clip(values, min=-reach, max=reach).astype(held_as)


def setup_inputs(seed: int = 0) -> dict:
    key_of = jax.random.split(jax.random.key(seed), 5)
    panel_t = gaussian(key_of[0], (S, B, R), R ** -0.5, 0.0625, ((0, 16), (2, 8)), jnp.float32)
    ancestor = draw_ancestor(jax.random.fold_in(key_of[4], 71), 0)
    structure = place_ends((jax.random.randint(key_of[2], (S, NA), 0, 4) < 3).astype(jnp.int32), jax.random.fold_in(key_of[2], 1), 0, 1)
    diag_inv = gaussian(key_of[3], (S, B, B), 1.0, 6.0, ((0, 16),), jnp.float32)
    return dict(panel_t=panel_t, ancestor=ancestor, structure=structure, diag_inv=diag_inv)


def reference(panel_t, ancestor, structure, diag_inv):
    mask = jnp.repeat(structure.astype(jnp.float32), B, axis=1)
    masked = panel_t * mask[:, None, :]
    flat = masked.reshape(S * B, R)
    inverse_panel = -jnp.dot(flat, ancestor, precision=lax.Precision.HIGHEST, preferred_element_type=jnp.float32)
    blocks = inverse_panel.reshape(S, B, R)
    inverse_diag = diag_inv - jnp.einsum("kbj,kcj->kbc", blocks, masked, precision=lax.Precision.HIGHEST)
    return inverse_panel, inverse_diag
```

```python
import functools

import jax
import jax.numpy as jnp
from jax import lax
from jax.experimental import pallas as pl
from jax.experimental.pallas import tpu as pltpu
from jax.sharding import PartitionSpec as P

MESH = pl.DeviceIdType.MESH
F32 = jnp.float32
BF16 = jnp.bfloat16

DX = (0, 0, -1, 1, 0, -1, 1, 0, 2, 2, -1, 1, 2, -1, 1, 2)
DZ = (0, 0, 0, 0, 1, 0, 0, 1, 0, 0, 1, 1, 1, 1, 1, 1)
TO_RIGHT = {0: 2, 1: 5, 2: 8, 4: 10, 7: 13}
TO_LEFT = {1: 3, 0: 6, 3: 9, 7: 11, 4: 14}
TO_Z = {0: 4, 1: 7, 8: 12, 9: 15}
EVENTS = 16
NX, NY, NZ = 4, 4, 2


def split(value):
    high = value.astype(BF16)
    low = (value - high.astype(F32)).astype(BF16)
    return high, low


def kernel(
    panel, ancestor, structure, diag_inv, panel_out, diag_out,
    gathered, b_high, b_low, a_high, a_low, partial, got1, got2, owned, got3, final, arrived, own_diag, got_diag, sum_diag,
    all_diag,
    gather_send, gather_recv, core_send, core_recv, send1, recv1, send2, recv2, send3, recv3, send4, recv4, send5, recv5,
    send6, recv6,
):
    row = lax.axis_index("prow")
    col = lax.axis_index("pcol")
    core = lax.rem(col, 2)
    zl = lax.rem(col // 2, 2)
    x = col // 4
    y = lax.rem(row, NY)
    zh = row // NY

    def at_col(xx, zz, cc):
        return (xx * 2 + zz) * 2 + cc

    right = (row, at_col(lax.rem(x + 1, NX), zl, core))
    left = (row, at_col(lax.rem(x + NX - 1, NX), zl, core))
    z_pair = (row, at_col(x, 1 - zl, core))
    twin = (row, at_col(x, zl, 1 - core))
    y_up, y_down, y_far = lax.rem(y + 1, NY), lax.rem(y + NY - 1, NY), lax.rem(y + 2, NY)
    up = (zh * NY + y_up, col)
    down = (zh * NY + y_down, col)
    z_far = ((1 - zh) * NY + y, col)
    home_row = col // 2
    mine_home = (home_row == row).astype(jnp.int32)

    barrier = pltpu.get_barrier_semaphore()

    def greet(device):
        pl.semaphore_signal(barrier, inc=1, device_id=device, device_id_type=MESH)

    for device in (right, left, z_pair, twin):
        greet(device)
    for step in range(1, 8):
        greet((lax.rem(row + step, 8), col))
    for other in range(8):
        for half in range(2):
            source = (other, 2 * row + half)

            @pl.when(jnp.logical_or(other != row, 2 * row + half != col))
            def _():
                greet(source)

    for n in range(2):
        high, low = split(ancestor[:, n * 256 : (n + 1) * 256])
        b_high[n] = high
        b_low[n] = low

    def load(unit, event, value):
        xx = lax.rem(x + NX + DX[event], NX)
        zz = zl if DZ[event] == 0 else 1 - zl
        cc = core if unit == 0 else 1 - core
        node = at_col(xx, zz, cc)
        for block in range(4):
            mask = structure[node, row * 4 + block].astype(F32)
            high, low = split(value[:, block * 256 : (block + 1) * 256] * mask)
            a_high[unit * 128 : (unit + 1) * 128, block * 256 : (block + 1) * 256] = high
            a_low[unit * 128 : (unit + 1) * 128, block * 256 : (block + 1) * 256] = low

    pl.semaphore_wait(barrier, 27 - mine_home)

    waits = []

    def send(source, target, send_sem, recv_sem, device):
        copy = pltpu.make_async_remote_copy(
            src_ref=source, dst_ref=target, send_sem=send_sem, recv_sem=recv_sem, device_id=device, device_id_type=MESH
        )
        copy.start()
        waits.append(copy)
        return copy

    def mine(event):
        if event < 2:
            return panel.at[0, pl.ds(event * 128, 128), :]
        return gathered.at[0, event]

    def wait_recv(target, send_sem, recv_sem):
        pltpu.make_async_remote_copy(
            src_ref=target, dst_ref=target, send_sem=send_sem, recv_sem=recv_sem, device_id=twin, device_id_type=MESH
        ).wait_recv()

    count = [0]

    def arrive(event):
        if event >= 2:
            wait_recv(gathered.at[0, event], gather_send.at[0], gather_recv.at[event])
        for table, device in ((TO_RIGHT, right), (TO_LEFT, left), (TO_Z, z_pair)):
            if event in table:
                there = table[event]
                send(mine(event), gathered.at[0, there], gather_send.at[count[0]], gather_recv.at[there], device)
                count[0] += 1
        send(mine(event), gathered.at[1, event], core_send.at[event], core_recv.at[event], twin)

    def multiply(event):
        load(0, event, mine(event))
        wait_recv(gathered.at[1, event], core_send.at[0], core_recv.at[event])
        load(1, event, gathered.at[1, event])

        @pl.loop(0, 2)
        def _(n):
            high = a_high[...]
            product = (
                jnp.dot(high, b_high[n], preferred_element_type=F32)
                + jnp.dot(high, b_low[n], preferred_element_type=F32)
                + jnp.dot(a_low[...], b_high[n], preferred_element_type=F32)
            )
            for unit in range(2):
                for yy in range(NY):
                    partial[event, yy, n, unit * 32 : (unit + 1) * 32, :] = product[unit * 128 + yy * 32 : unit * 128 + yy * 32 + 32, :]

        send(partial.at[event, y_far, 0], got1.at[event, 0], send1.at[event, 0], recv1.at[event, 0], up)
        send(partial.at[event, y_far, 1], got1.at[event, 1], send1.at[event, 1], recv1.at[event, 1], down)

    def stage2(event):
        for way, (yy, device) in enumerate(((y_up, up), (y_down, down))):
            wait_recv(got1.at[event, way], send1.at[event, way], recv1.at[event, way])
            partial[event, yy, way] += got1[event, way]
            send(partial.at[event, yy], got2.at[event, way], send2.at[event, way], recv2.at[event, way], device)

    def stage3(event):
        for way in range(2):
            wait_recv(got2.at[event, way], send2.at[event, way], recv2.at[event, way])
        for n in range(2):
            total = partial[event, y, n] + got2[event, 0, n] + got2[event, 1, n]
            for unit in range(2):
                for hz in range(2):
                    start = unit * 32 + hz * 16
                    owned[event, hz, unit, :, n * 256 : (n + 1) * 256] = total[start : start + 16, :]
        send(owned.at[event, 1 - zh], got3.at[event], send3.at[event], recv3.at[event], z_far)

    def home(event, unit):
        xx = lax.rem(x + NX + DX[event], NX)
        zz = zl if DZ[event] == 0 else 1 - zl
        cc = core if unit == 0 else 1 - core
        return at_col(xx, zz, cc)

    def stage4(event):
        wait_recv(got3.at[event], send3.at[event], recv3.at[event])
        final[event] = owned[event, zh] + got3[event]
        half = event % 2
        start = pl.multiple_of(half * 128 + y * 32 + zh * 16, 16)
        for unit in range(2):
            node = home(event, unit)
            here = jnp.logical_and(home_row == row, node == col)
            target = arrived.at[core, pl.ds(start, 16), :]

            @pl.when(here)
            def _():
                arrived[core, pl.ds(start, 16), :] = final[event, unit]

            @pl.when(jnp.logical_not(here))
            def _():
                pltpu.make_async_remote_copy(
                    src_ref=final.at[event, unit], dst_ref=target, send_sem=send4.at[event, unit],
                    recv_sem=recv4.at[core, half, row], device_id=(home_row, node), device_id_type=MESH,
                ).start()

    for step in range(EVENTS + 3):
        if step < EVENTS:
            arrive(step)
            multiply(step)
        if 0 <= step - 1 < EVENTS:
            stage2(step - 1)
        if 0 <= step - 2 < EVENTS:
            stage3(step - 2)
        if 0 <= step - 3 < EVENTS:
            stage4(step - 3)

    for side in range(2):
        for half in range(2):
            for source in range(8):
                start = half * 128 + (source % 4) * 32 + (source // 4) * 16
                there = jnp.logical_and(source == row, 2 * row + side == col)

                @pl.when(jnp.logical_not(there))
                def _():
                    wait_recv(arrived.at[side, start : start + 16, :], send4.at[0, 0], recv4.at[side, half, source])

    for block in range(4):
        mask = structure[col, row * 4 + block].astype(F32)
        high, low = split(panel[0, :, block * 256 : (block + 1) * 256] * mask)
        a_high[:, block * 256 : (block + 1) * 256] = high
        a_low[:, block * 256 : (block + 1) * 256] = low
    contract = functools.partial(
        lax.dot_general, dimension_numbers=(((1,), (1,)), ((), ())), preferred_element_type=F32
    )
    total = jnp.zeros((256, 256), F32)
    for side in range(2):
        value = -arrived[side]
        panel_out[:, side * 512 : (side + 1) * 512] = value
        high, low = split(value)
        right_high = a_high[:, side * 512 : (side + 1) * 512]
        right_low = a_low[:, side * 512 : (side + 1) * 512]
        total = total + contract(high, right_high) + contract(high, right_low) + contract(low, right_high)
    own_diag[...] = total
    for step in range(1, 8):
        other = lax.rem(row + step, 8)
        piece = pl.ds(pl.multiple_of(other * 32, 32), 32)
        send(own_diag.at[piece, :], got_diag.at[row], send5.at[step], recv5.at[row], (other, col))
    here = pl.ds(pl.multiple_of(row * 32, 32), 32)
    result = diag_inv[0, here, :] - own_diag[here, :]
    for step in range(1, 8):
        other = lax.rem(row + step, 8)
        wait_recv(got_diag.at[other], send5.at[step], recv5.at[other])
        result = result - got_diag[other]
    sum_diag[...] = result
    for step in range(1, 8):
        other = lax.rem(row + step, 8)
        send(sum_diag, all_diag.at[row], send6.at[step], recv6.at[row], (other, col))
    diag_out[0, here, :] = result
    for step in range(1, 8):
        other = lax.rem(row + step, 8)
        wait_recv(all_diag.at[other], send6.at[step], recv6.at[other])
        diag_out[0, pl.ds(pl.multiple_of(other * 32, 32), 32), :] = all_diag[other]

    for copy in waits:
        copy.wait_send()
    for event in range(EVENTS):
        for unit in range(2):
            node = home(event, unit)

            @pl.when(jnp.logical_or(home_row != row, node != col))
            def _():
                pltpu.make_async_remote_copy(
                    src_ref=final.at[event, unit], dst_ref=final.at[event, unit], send_sem=send4.at[event, unit],
                    recv_sem=recv4.at[0, 0, 0], device_id=twin, device_id_type=MESH,
                ).wait_send()


def local(panel_t, ancestor, structure, diag_inv):
    vmem = pltpu.VMEM
    dma = pltpu.SemaphoreType.DMA
    return pl.pallas_call(
        kernel,
        out_shape=(
            jax.ShapeDtypeStruct((256, 1024), F32),
            jax.ShapeDtypeStruct((1, 256, 256), F32),
        ),
        in_specs=[
            pl.BlockSpec(memory_space=vmem),
            pl.BlockSpec(memory_space=vmem),
            pl.BlockSpec(memory_space=pltpu.SMEM),
            pl.BlockSpec(memory_space=vmem),
        ],
        out_specs=(pl.BlockSpec(memory_space=vmem), pl.BlockSpec(memory_space=vmem)),
        scratch_shapes=[
            vmem((2, EVENTS, 128, 1024), F32),
            vmem((2, 1024, 256), BF16),
            vmem((2, 1024, 256), BF16),
            vmem((256, 1024), BF16),
            vmem((256, 1024), BF16),
            vmem((EVENTS, NY, 2, 64, 256), F32),
            vmem((EVENTS, 2, 64, 256), F32),
            vmem((EVENTS, 2, 2, 64, 256), F32),
            vmem((EVENTS, 2, 2, 16, 512), F32),
            vmem((EVENTS, 2, 16, 512), F32),
            vmem((EVENTS, 2, 16, 512), F32),
            vmem((2, 256, 512), F32),
            vmem((256, 256), F32),
            vmem((8, 32, 256), F32),
            vmem((32, 256), F32),
            vmem((8, 32, 256), F32),
            dma((14,)),
            dma((EVENTS,)),
            dma((EVENTS,)),
            dma((EVENTS,)),
            dma((EVENTS, 2)),
            dma((EVENTS, 2)),
            dma((EVENTS, 2)),
            dma((EVENTS, 2)),
            dma((EVENTS,)),
            dma((EVENTS,)),
            dma((EVENTS, 2)),
            dma((2, 2, 8)),
            dma((8,)),
            dma((8,)),
            dma((8,)),
            dma((8,)),
        ],
        compiler_params=pltpu.CompilerParams(
            collective_id=0, has_side_effects=True, vmem_limit_bytes=60 * 1024 * 1024
        ),
        name="level_update",
    )(panel_t, ancestor, structure, diag_inv)


def solution(mesh):
    return jax.shard_map(
        local,
        mesh=mesh,
        in_specs=(P("pcol", None, "prow"), P("prow", "pcol"), P(), P("pcol", None, None)),
        out_specs=(P("pcol", "prow"), P("pcol", None, None)),
        check_vma=False,
    )
```

```python
import functools

import jax
import jax.numpy as jnp
from jax import lax
from jax.experimental import pallas as pl
from jax.experimental.pallas import tpu as pltpu
from jax.sharding import PartitionSpec as P

MESH = pl.DeviceIdType.MESH
F32 = jnp.float32
BF16 = jnp.bfloat16

DX = (0, 0, -1, 1, 1, -1, 2, 2)
EVENTS = 8
TO_RIGHT = {0: 2, 1: 5, 2: 6}
TO_LEFT = {1: 3, 0: 4, 3: 7}
PAIRS = ((0, 1), (2, 5), (4, 3), (6, 7))
ITEMS = 16
ORDER = (
    "M0 M1 A0 B0", "A1 B1 C0 F2", "F3 M2 M3 C1", "A2 B2 A3 B3", "F5 F4 G2 M8", "C2 M5 M4 M9",
    "M10 A5 A8 B5", "B8 A4 B4 C3", "A9 F6 F7 B9", "A10 B10 M6 M7", "M11 C5 C8 C4", "G3 M12 M13 M14",
    "M15 A6 B6 D0", "A7 B7 D1 D2", "D3 D5 C9 A11", "B11 C10 D8 A12", "B12 D4 A13 B13", "A14 B14 A15 B15",
    "D9 C6 D10 C7", "D6 D7 C11 C12", "D11 C13 D12 C14", "D13 C15 D14 D15",
)
NX, NY = 4, 4
WINDOWS = (8, 4, 4)
PACE = 2


def parts(item):
    if item < EVENTS:
        return ((item, 0), (item, 1))
    first, second = PAIRS[(item - EVENTS) % 4]
    block = 2 + (item - EVENTS) // 4
    return ((first, block), (second, block))


def split(value):
    high = value.astype(BF16)
    low = (value - high.astype(F32)).astype(BF16)
    return high, low


def pick(table, index):
    value = jnp.int32(table[0])
    for place in range(1, len(table)):
        value = jnp.where(index == place, jnp.int32(table[place]), value)
    return value


def kernel(
    panel, ancestor, structure, diag_inv, panel_out, diag_out,
    gathered, b_pair, b_high, b_low, a_high, a_low, partial, got1, got2, owned, got3, final, arrived, own_diag, got_diag,
    sum_diag, all_diag,
    gather_send, gather_recv, core_send, core_recv, pair_send, pair_recv, send1, recv1, send2, recv2, send3, recv3, send4, recv4,
    send5, recv5, send6, recv6,
):
    row = lax.axis_index("prow")
    col = lax.axis_index("pcol")
    core = lax.rem(col, 2)
    zl = lax.rem(col // 2, 2)
    x = col // 4
    y = lax.rem(row, NY)
    zh = row // NY

    def at_col(xx, zz, cc):
        return (xx * 2 + zz) * 2 + cc

    right = (row, at_col(lax.rem(x + 1, NX), zl, core))
    left = (row, at_col(lax.rem(x + NX - 1, NX), zl, core))
    z_pair = (row, at_col(x, 1 - zl, core))
    twin = (row, at_col(x, zl, 1 - core))
    y_up, y_down, y_far = lax.rem(y + 1, NY), lax.rem(y + NY - 1, NY), lax.rem(y + 2, NY)
    up = (zh * NY + y_up, col)
    down = (zh * NY + y_down, col)
    z_far = ((1 - zh) * NY + y, col)
    home_rows = (x * 2 + zl, x * 2 + 1 - zl)
    mine_home = (row // 2 == x).astype(jnp.int32)

    barrier = pltpu.get_barrier_semaphore()

    def greet(device):
        pl.semaphore_signal(barrier, inc=1, device_id=device, device_id_type=MESH)

    for device in (right, left, z_pair, twin):
        greet(device)
    for step in range(1, 8):
        greet((lax.rem(row + step, 8), col))
    for other in range(8):
        for side in range(2):
            source = at_col(row // 2, zl, side)

            @pl.when(jnp.logical_or(other != row, source != col))
            def _():
                greet((other, source))

    def take_columns(block, value):
        high, low = split(value)
        b_high[block] = high
        b_low[block] = low

    for block in range(2):
        take_columns(block, ancestor[:, block * 256 : (block + 1) * 256])

    pl.semaphore_wait(barrier, 27 - mine_home)

    waits = []

    def send(source, target, send_sem, recv_sem, device):
        copy = pltpu.make_async_remote_copy(
            src_ref=source, dst_ref=target, send_sem=send_sem, recv_sem=recv_sem, device_id=device, device_id_type=MESH
        )
        copy.start()
        waits.append(copy)

    def wait_recv(target, send_sem, recv_sem):
        pltpu.make_async_remote_copy(
            src_ref=target, dst_ref=target, send_sem=send_sem, recv_sem=recv_sem, device_id=twin, device_id_type=MESH
        ).wait_recv()

    def mine(event):
        if event < 2:
            return panel.at[0, pl.ds(event * 128, 128), :]
        return gathered.at[0, event]

    count = [0]

    def pass_on(event, table, device):
        if event in table:
            there = table[event]
            send(mine(event), gathered.at[0, there], gather_send.at[count[0]], gather_recv.at[there], device)
            count[0] += 1

    def to_twin(event):
        send(mine(event), gathered.at[1, event], core_send.at[event], core_recv.at[event], twin)

    def arrive(event):
        wait_recv(gathered.at[0, event], gather_send.at[0], gather_recv.at[event])
        pass_on(event, TO_RIGHT, right)
        pass_on(event, TO_LEFT, left)
        to_twin(event)

    def take_pair(block):
        wait_recv(b_pair.at[block - 2], pair_send.at[block - 2], pair_recv.at[block - 2])
        take_columns(block, b_pair[block - 2])

    def home_node(dx, unit):
        return at_col(lax.rem(x + NX + dx, NX), zl, core if unit == 0 else 1 - core)

    def load(event, unit, value):
        node = home_node(DX[event], unit)
        for block in range(4):
            mask = structure[node, row * 4 + block].astype(F32)
            high, low = split(value[:, block * 256 : (block + 1) * 256] * mask)
            a_high[event, unit * 128 : (unit + 1) * 128, block * 256 : (block + 1) * 256] = high
            a_low[event, unit * 128 : (unit + 1) * 128, block * 256 : (block + 1) * 256] = low

    def multiply(item):
        if item < EVENTS:
            load(item, 0, mine(item))
            wait_recv(gathered.at[1, item], core_send.at[0], core_recv.at[item])
            load(item, 1, gathered.at[1, item])
        (event0, block0), (event1, block1) = parts(item)

        @pl.loop(0, 2)
        def _(n):
            event = event0 + n * (event1 - event0)
            block = block0 + n * (block1 - block0)
            high = a_high[event]
            product = (
                jnp.dot(high, b_high[block], preferred_element_type=F32)
                + jnp.dot(high, b_low[block], preferred_element_type=F32)
                + jnp.dot(a_low[event], b_high[block], preferred_element_type=F32)
            )
            for unit in range(2):
                for yy in range(NY):
                    start = unit * 128 + yy * 32
                    partial[item, yy, n, unit * 32 : (unit + 1) * 32, :] = product[start : start + 32, :]

        send(partial.at[item, y_far, 0], got1.at[item, 0], send1.at[item, 0], recv1.at[item, 0], up)
        send(partial.at[item, y_far, 1], got1.at[item, 1], send1.at[item, 1], recv1.at[item, 1], down)

    def stage2(item, way):
        yy, device = ((y_up, up), (y_down, down))[way]
        wait_recv(got1.at[item, way], send1.at[item, way], recv1.at[item, way])
        partial[item, yy, way] += got1[item, way]
        send(partial.at[item, yy], got2.at[item, way], send2.at[item, way], recv2.at[item, way], device)

    def stage3(item):
        for way in range(2):
            wait_recv(got2.at[item, way], send2.at[item, way], recv2.at[item, way])
        for n in range(2):
            total = partial[item, y, n] + got2[item, 0, n] + got2[item, 1, n]
            for unit in range(2):
                for hz in range(2):
                    start = unit * 32 + hz * 16
                    owned[item, hz, unit, n] = total[start : start + 16, :]
        send(owned.at[item, 1 - zh], got3.at[item], send3.at[item], recv3.at[item], z_far)

    def stage4(item):
        wait_recv(got3.at[item], send3.at[item], recv3.at[item])
        final[item] = owned[item, zh] + got3[item]

    def send_piece(item, dx, own, place, unit, act):
        node = home_node(dx, unit)
        home_row = home_rows[0] if own else home_rows[1]
        here = jnp.logical_and(home_row == row, node == col)
        start = pl.multiple_of(y * 32 + zh * 16, 16)
        if own:
            target = arrived.at[core, :, place, pl.ds(start, 16), :]
        else:
            target = arrived.at[core, place, :, pl.ds(start, 16), :]
        copy = pltpu.make_async_remote_copy(
            src_ref=final.at[item, unit], dst_ref=target, send_sem=send4.at[item, unit], recv_sem=recv4.at[core, place, row],
            device_id=(home_row, node), device_id_type=MESH,
        )
        if act:

            @pl.when(here)
            def _():
                if own:
                    arrived[core, :, place, pl.ds(start, 16), :] = final[item, unit]
                else:
                    arrived[core, place, :, pl.ds(start, 16), :] = final[item, unit]

        @pl.when(jnp.logical_not(here))
        def _():
            if act:
                copy.start()
            else:
                copy.wait_send()

    ITEM_DX = DX + tuple(DX[parts(item)[0][0]] for item in range(EVENTS, ITEMS))

    def send_home(items, turn):
        item = pick(items, lax.rem(row + turn, len(items)))
        dx = pick(ITEM_DX, item)
        for unit in range(2):

            @pl.when(item < EVENTS)
            def _():
                send_piece(item, dx, True, lax.rem(item, 2), unit, True)

            @pl.when(item >= EVENTS)
            def _():
                send_piece(item, dx, False, (item - EVENTS) // 4, unit, True)

    pass_on(0, TO_RIGHT, right)
    pass_on(1, TO_LEFT, left)
    for block in range(2):
        send(ancestor.at[:, pl.ds(block * 256, 256)], b_pair.at[block], pair_send.at[block], pair_recv.at[block], z_pair)
    to_twin(0)
    to_twin(1)
    pass_on(1, TO_RIGHT, right)
    pass_on(0, TO_LEFT, left)
    work = {
        "F": arrive,
        "G": take_pair,
        "M": multiply,
        "A": lambda item: stage2(item, 0),
        "B": lambda item: stage2(item, 1),
        "C": stage3,
        "D": stage4,
    }
    batch, ready, sizes = [], [], list(WINDOWS)
    for step in " ".join(ORDER).split():
        item = int(step[1:])
        work[step[0]](item)
        if step[0] == "D":
            batch.append(item)
            for _ in range(min(PACE, len(ready))):
                send_home(*ready.pop(0))
            if len(batch) == sizes[0]:
                ready += [(tuple(batch), turn) for turn in range(len(batch))]
                batch = []
                sizes.pop(0)
    for items, turn in ready:
        send_home(items, turn)

    for block in range(4):
        mask = structure[col, row * 4 + block].astype(F32)
        high, low = split(panel[0, :, block * 256 : (block + 1) * 256] * mask)
        a_high[0, :, block * 256 : (block + 1) * 256] = high
        a_low[0, :, block * 256 : (block + 1) * 256] = low

    for side in range(2):
        for place in range(2):
            for source in range(8):
                there = jnp.logical_and(source == row, at_col(row // 2, zl, side) == col)

                @pl.when(jnp.logical_not(there))
                def _():
                    wait_recv(final.at[0, 0], send4.at[0, 0], recv4.at[side, place, source])

    contract = functools.partial(
        lax.dot_general, dimension_numbers=(((1,), (1,)), ((), ())), preferred_element_type=F32
    )
    total = jnp.zeros((256, 256), F32)
    for side in range(2):
        for block in range(2):
            columns = slice(side * 512 + block * 256, side * 512 + block * 256 + 256)
            value = -arrived[side, block].reshape(256, 256)
            panel_out[:, columns] = value
            high, low = split(value)
            right_high = a_high[0, :, columns]
            right_low = a_low[0, :, columns]
            total = total + contract(high, right_high) + contract(high, right_low) + contract(low, right_high)
    own_diag[...] = total
    for step in range(1, 8):
        other = lax.rem(row + step, 8)
        piece = pl.ds(pl.multiple_of(other * 32, 32), 32)
        send(own_diag.at[piece, :], got_diag.at[row], send5.at[step], recv5.at[row], (other, col))
    here = pl.ds(pl.multiple_of(row * 32, 32), 32)
    result = diag_inv[0, here, :] - own_diag[here, :]
    for step in range(1, 8):
        other = lax.rem(row + step, 8)
        wait_recv(got_diag.at[other], send5.at[step], recv5.at[other])
        result = result - got_diag[other]
    sum_diag[...] = result
    for step in range(1, 8):
        other = lax.rem(row + step, 8)
        send(sum_diag, all_diag.at[row], send6.at[step], recv6.at[row], (other, col))
    diag_out[0, here, :] = result
    for step in range(1, 8):
        other = lax.rem(row + step, 8)
        wait_recv(all_diag.at[other], send6.at[step], recv6.at[other])
        diag_out[0, pl.ds(pl.multiple_of(other * 32, 32), 32), :] = all_diag[other]

    for copy in waits:
        copy.wait_send()
    for item in range(ITEMS):
        for unit in range(2):
            own = item < EVENTS
            place = item % 2 if own else (item - EVENTS) // 4
            send_piece(item, ITEM_DX[item], own, place, unit, False)


def local(panel_t, ancestor, structure, diag_inv):
    vmem = pltpu.VMEM
    dma = pltpu.SemaphoreType.DMA
    return pl.pallas_call(
        kernel,
        out_shape=(
            jax.ShapeDtypeStruct((256, 1024), F32),
            jax.ShapeDtypeStruct((1, 256, 256), F32),
        ),
        in_specs=[
            pl.BlockSpec(memory_space=vmem),
            pl.BlockSpec(memory_space=vmem),
            pl.BlockSpec(memory_space=pltpu.SMEM),
            pl.BlockSpec(memory_space=vmem),
        ],
        out_specs=(pl.BlockSpec(memory_space=vmem), pl.BlockSpec(memory_space=vmem)),
        scratch_shapes=[
            vmem((2, EVENTS, 128, 1024), F32),
            vmem((2, 1024, 256), F32),
            vmem((4, 1024, 256), BF16),
            vmem((4, 1024, 256), BF16),
            vmem((EVENTS, 256, 1024), BF16),
            vmem((EVENTS, 256, 1024), BF16),
            vmem((ITEMS, NY, 2, 64, 256), F32),
            vmem((ITEMS, 2, 64, 256), F32),
            vmem((ITEMS, 2, 2, 64, 256), F32),
            vmem((ITEMS, 2, 2, 2, 16, 256), F32),
            vmem((ITEMS, 2, 2, 16, 256), F32),
            vmem((ITEMS, 2, 2, 16, 256), F32),
            vmem((2, 2, 2, 128, 256), F32),
            vmem((256, 256), F32),
            vmem((8, 32, 256), F32),
            vmem((32, 256), F32),
            vmem((8, 32, 256), F32),
            dma((6,)),
            dma((EVENTS,)),
            dma((EVENTS,)),
            dma((EVENTS,)),
            dma((2,)),
            dma((2,)),
            dma((ITEMS, 2)),
            dma((ITEMS, 2)),
            dma((ITEMS, 2)),
            dma((ITEMS, 2)),
            dma((ITEMS,)),
            dma((ITEMS,)),
            dma((ITEMS, 2)),
            dma((2, 2, 8)),
            dma((8,)),
            dma((8,)),
            dma((8,)),
            dma((8,)),
        ],
        compiler_params=pltpu.CompilerParams(
            collective_id=0, has_side_effects=True, vmem_limit_bytes=60 * 1024 * 1024
        ),
        name="level_update",
    )(panel_t, ancestor, structure, diag_inv)


def solution(mesh):
    return jax.shard_map(
        local,
        mesh=mesh,
        in_specs=(P("pcol", None, "prow"), P("prow", "pcol"), P(), P("pcol", None, None)),
        out_specs=(P("pcol", "prow"), P("pcol", None, None)),
        check_vma=False,
    )
```

```python
import functools

import jax
import jax.numpy as jnp
from jax import lax
from jax.experimental import pallas as pl
from jax.experimental.pallas import tpu as pltpu
from jax.sharding import PartitionSpec as P

MESH = pl.DeviceIdType.MESH
F32 = jnp.float32
BF16 = jnp.bfloat16

DX = (0, 0, 0, 0, -1, -1, 1, 1, -1, -1, 1, 1, 2, 2, 2, 2)
QUARTER = (0, 1, 2, 3, 0, 1, 3, 2, 2, 3, 1, 0, 0, 1, 3, 2)
EVENTS = 16
TO_RIGHT = {0: 4, 1: 5, 2: 8, 3: 9, 4: 12, 5: 13}
TO_LEFT = {3: 6, 2: 7, 1: 10, 0: 11, 6: 14, 7: 15}
PAIRS = ((0, 1), (2, 3), (4, 5), (7, 6), (8, 9), (11, 10), (12, 13), (15, 14))
ITEMS = 32
ORDER = (
    "M0 M1 M2 M3", "A0 B0 A1 B1", "F4 F6 A2 B2", "A3 B3 M4 M6", "C0 C1 F5 F7", "C2 C3 M5 A4",
    "A6 B4 B6 M7", "F8 F10 A5 B5", "C4 M8 M10 A7", "B7 C6 C5 F9", "F11 A8 B8 G2", "M16 A10 B10 M9",
    "M11 M17 A16 B16", "M18 F12 F14 M19", "A9 B9 A11 B11", "M20 A17 B17 M12", "M14 A18 F13 F15", "A19 B18 B19 M21",
    "C7 C8 M13 M15", "A20 B20 M22 M23", "A12 A14 B12 B14", "C9 C10 C11 C16", "C17 C18 C19 A21", "B21 A13 B13 A15",
    "B15 G3 M24 M25", "A22 A23 B22 B23", "M26 M27 M28 M29", "M30 M31 D0 D1", "D2 D3 D4 D5", "D6 D7 D8 D9",
    "D10 D11 C12 D16", "A24 B24 C13 D17", "C14 A25 B25 C15", "D18 C20 C21 D19", "C22 C23 A26 B26", "A27 B27 A28 B28",
    "A29 B29 D12 A30", "B30 A31 B31 D13", "D14 D15 D20 D21", "D22 D23 C24 C25", "D24 C26 C27 D25", "C28 D26 C29 D27",
    "C30 D28 C31 D29", "D30 D31",
)
NX, NY = 4, 4
WINDOWS = (16, 8, 8)
PACE = 2


def parts(item):
    if item < EVENTS:
        return ((item, 0), (item, 1))
    first, second = PAIRS[(item - EVENTS) % 8]
    block = 2 + (item - EVENTS) // 8
    return ((first, block), (second, block))


def split(value):
    high = value.astype(BF16)
    low = (value - high.astype(F32)).astype(BF16)
    return high, low


def pick(table, index):
    value = jnp.int32(table[0])
    for place in range(1, len(table)):
        value = jnp.where(index == place, jnp.int32(table[place]), value)
    return value


def kernel(
    panel_hbm, ancestor_hbm, structure, diag_hbm, panel_out, diag_out,
    panel, ancestor, diag_inv, gathered, b_pair, b_high, b_low, a_high, a_low, own_high, own_low, partial, got1, got2, owned, got3, final, arrived, own_diag, got_diag,
    sum_diag, all_diag,
    gather_send, gather_recv, core_send, core_recv, pair_send, pair_recv, send1, recv1, send2, recv2, send3, recv3, send4, recv4,
    send5, recv5, send6, recv6, load_sem,
):
    row = lax.axis_index("prow")
    col = lax.axis_index("pcol")
    core = lax.rem(col, 2)
    zl = lax.rem(col // 2, 2)
    x = col // 4
    y = lax.rem(row, NY)
    zh = row // NY

    def at_col(xx, zz, cc):
        return (xx * 2 + zz) * 2 + cc

    right = (row, at_col(lax.rem(x + 1, NX), zl, core))
    left = (row, at_col(lax.rem(x + NX - 1, NX), zl, core))
    z_pair = (row, at_col(x, 1 - zl, core))
    twin = (row, at_col(x, zl, 1 - core))
    y_up, y_down, y_far = lax.rem(y + 1, NY), lax.rem(y + NY - 1, NY), lax.rem(y + 2, NY)
    up = (zh * NY + y_up, col)
    down = (zh * NY + y_down, col)
    z_far = ((1 - zh) * NY + y, col)
    home_rows = (x * 2 + zl, x * 2 + 1 - zl)

    barrier = pltpu.get_barrier_semaphore()

    def greet(device):
        pl.semaphore_signal(barrier, inc=1, device_id=device, device_id_type=MESH)

    greeted = (right, left, z_pair, twin, up, down, z_far)
    for device in greeted:
        greet(device)

    copies = [
        pltpu.make_async_copy(panel_hbm, panel, load_sem.at[0]),
        pltpu.make_async_copy(ancestor_hbm, ancestor, load_sem.at[1]),
        pltpu.make_async_copy(diag_hbm, diag_inv, load_sem.at[2]),
    ]
    for copy in copies:
        copy.start()
    for copy in copies:
        copy.wait()

    def take_columns(block, value):
        high, low = split(value)
        b_high[block] = high
        b_low[block] = low

    for block in range(2):
        take_columns(block, ancestor[:, block * 256 : (block + 1) * 256])

    def home_node(dx, unit):
        return at_col(lax.rem(x + NX + dx, NX), zl, core if unit == 0 else 1 - core)

    def load(event, unit, value):
        node = home_node(DX[event], unit)
        for block in range(4):
            mask = structure[node, row * 4 + block].astype(F32)
            high, low = split(value[:, block * 256 : (block + 1) * 256] * mask)
            a_high[event, unit * 64 : (unit + 1) * 64, block * 256 : (block + 1) * 256] = high
            a_low[event, unit * 64 : (unit + 1) * 64, block * 256 : (block + 1) * 256] = low

    for event in range(4):
        load(event, 0, panel[0, event * 64 : (event + 1) * 64, :])

    pl.semaphore_wait(barrier, len(greeted))

    sent = []

    def send(source, target, send_sem, recv_sem, device):
        copy = pltpu.make_async_remote_copy(
            src_ref=source, dst_ref=target, send_sem=send_sem, recv_sem=recv_sem, device_id=device, device_id_type=MESH
        )
        copy.start()
        sent.append(copy)

    def wait_recv(target, send_sem, recv_sem):
        pltpu.make_async_remote_copy(
            src_ref=target, dst_ref=target, send_sem=send_sem, recv_sem=recv_sem, device_id=twin, device_id_type=MESH
        ).wait_recv()

    def mine(event):
        if event < 4:
            return panel.at[0, pl.ds(event * 64, 64), :]
        return gathered.at[0, event]

    count = [0]

    def pass_on(event, table, device):
        if event in table:
            there = table[event]
            send(mine(event), gathered.at[0, there], gather_send.at[count[0]], gather_recv.at[there], device)
            count[0] += 1

    def to_twin(event):
        send(mine(event), gathered.at[1, event], core_send.at[event], core_recv.at[event], twin)

    def arrive(event):
        wait_recv(gathered.at[0, event], gather_send.at[0], gather_recv.at[event])
        pass_on(event, TO_RIGHT, right)
        pass_on(event, TO_LEFT, left)
        to_twin(event)

    def take_pair(block):
        wait_recv(b_pair.at[block - 2], pair_send.at[block - 2], pair_recv.at[block - 2])
        take_columns(block, b_pair[block - 2])

    def multiply(item):
        if item < EVENTS:
            if item >= 4:
                load(item, 0, mine(item))
            wait_recv(gathered.at[1, item], core_send.at[0], core_recv.at[item])
            load(item, 1, gathered.at[1, item])
        (event0, block0), (event1, block1) = parts(item)

        @pl.loop(0, 2)
        def _(n):
            event = event0 + n * (event1 - event0)
            block = block0 + n * (block1 - block0)
            high = a_high[event]
            product = (
                jnp.dot(high, b_high[block], preferred_element_type=F32)
                + jnp.dot(high, b_low[block], preferred_element_type=F32)
                + jnp.dot(a_low[event], b_high[block], preferred_element_type=F32)
            )
            for unit in range(2):
                for yy in range(NY):
                    start = unit * 64 + yy * 16
                    partial[item, yy, n, unit * 16 : (unit + 1) * 16, :] = product[start : start + 16, :]

        send(partial.at[item, y_far, 0], got1.at[item, 0], send1.at[item, 0], recv1.at[item, 0], up)
        send(partial.at[item, y_far, 1], got1.at[item, 1], send1.at[item, 1], recv1.at[item, 1], down)

    def stage2(item, way):
        yy, device = ((y_up, up), (y_down, down))[way]
        wait_recv(got1.at[item, way], send1.at[item, way], recv1.at[item, way])
        partial[item, yy, way] += got1[item, way]
        send(partial.at[item, yy], got2.at[item, way], send2.at[item, way], recv2.at[item, way], device)

    def stage3(item):
        for way in range(2):
            wait_recv(got2.at[item, way], send2.at[item, way], recv2.at[item, way])
        for n in range(2):
            total = partial[item, y, n] + got2[item, 0, n] + got2[item, 1, n]
            for unit in range(2):
                for hz in range(2):
                    start = unit * 16 + hz * 8
                    owned[item, hz, unit, n] = total[start : start + 8, :]
        send(owned.at[item, 1 - zh], got3.at[item], send3.at[item], recv3.at[item], z_far)

    def stage4(item):
        wait_recv(got3.at[item], send3.at[item], recv3.at[item])
        final[item] = owned[item, zh] + got3[item]

    def send_piece(item, dx, own, place, unit, act):
        node = home_node(dx, unit)
        home_row = home_rows[0] if own else home_rows[1]
        here = jnp.logical_and(home_row == row, node == col)
        rows = pl.ds(pl.multiple_of(y * 16 + zh * 8, 8), 8)
        if own:
            target = arrived.at[core, :, place, rows, :]
        else:
            quarters = pl.ds(lax.rem(place, 2) * 2, 2)
            target = arrived.at[core, place // 2, quarters, rows, :]
        copy = pltpu.make_async_remote_copy(
            src_ref=final.at[item, unit], dst_ref=target, send_sem=send4.at[item, unit], recv_sem=recv4.at[core, place, row],
            device_id=(home_row, node), device_id_type=MESH,
        )
        if act:

            @pl.when(here)
            def _():
                if own:
                    arrived[core, :, place, rows, :] = final[item, unit]
                else:
                    arrived[core, place // 2, quarters, rows, :] = final[item, unit]

        @pl.when(jnp.logical_not(here))
        def _():
            if act:
                copy.start()
            else:
                copy.wait_send()

    ITEM_DX = DX + tuple(DX[parts(item)[0][0]] for item in range(EVENTS, ITEMS))
    ITEM_PLACE = QUARTER + tuple(
        (parts(item)[0][1] - 2) * 2 + QUARTER[parts(item)[0][0]] // 2 for item in range(EVENTS, ITEMS)
    )

    def send_home(items, turn):
        item = pick(items, lax.rem(row + turn, len(items)))
        dx = pick(ITEM_DX, item)
        place = pick(ITEM_PLACE, item)
        for unit in range(2):

            @pl.when(item < EVENTS)
            def _():
                send_piece(item, dx, True, place, unit, True)

            @pl.when(item >= EVENTS)
            def _():
                send_piece(item, dx, False, place, unit, True)

    for turn in range(2):
        pass_on(turn, TO_RIGHT, right)
        pass_on(3 - turn, TO_LEFT, left)
    for block in range(2):
        send(ancestor.at[:, pl.ds(block * 256, 256)], b_pair.at[block], pair_send.at[block], pair_recv.at[block], z_pair)
    for event in range(4):
        to_twin(event)
    for turn in range(2, 4):
        pass_on(turn, TO_RIGHT, right)
        pass_on(3 - turn, TO_LEFT, left)
    work = {
        "F": arrive,
        "G": take_pair,
        "M": multiply,
        "A": lambda item: stage2(item, 0),
        "B": lambda item: stage2(item, 1),
        "C": stage3,
        "D": stage4,
    }
    batch, ready, sizes = [], [], list(WINDOWS)
    for step in " ".join(ORDER).split():
        item = int(step[1:])
        work[step[0]](item)
        if step[0] == "D":
            batch.append(item)
            for _ in range(min(PACE, len(ready))):
                send_home(*ready.pop(0))
            if len(batch) == sizes[0]:
                ready += [(tuple(batch), turn) for turn in range(len(batch))]
                batch = []
                sizes.pop(0)
    for items, turn in ready:
        send_home(items, turn)

    for block in range(4):
        mask = structure[col, row * 4 + block].astype(F32)
        high, low = split(panel[0, :, block * 256 : (block + 1) * 256] * mask)
        own_high[:, block * 256 : (block + 1) * 256] = high
        own_low[:, block * 256 : (block + 1) * 256] = low

    contract = functools.partial(
        lax.dot_general, dimension_numbers=(((1,), (1,)), ((), ())), preferred_element_type=F32
    )
    from_own = lax.rem(row, 2) == zl

    def take(side, place):
        for source in range(8):
            there = jnp.logical_and(source == row, at_col(row // 2, zl, side) == col)

            @pl.when(jnp.logical_not(there))
            def _():
                wait_recv(final.at[0, 0], send4.at[0, 0], recv4.at[side, place, source])

    total = jnp.zeros((256, 256), F32)
    for block in range(2):
        for side in range(2):
            for half in range(2):
                take_now = (block * 2 + half,)

                @pl.when(jnp.logical_not(from_own))
                def _():
                    take(side, take_now[0])

            if block == 0:

                @pl.when(from_own)
                def _():
                    for place in range(4):
                        take(side, place)

            columns = slice(side * 512 + block * 256, side * 512 + block * 256 + 256)
            value = arrived[side, block].reshape(256, 256)
            panel_out[:, columns] = value
            high, low = split(value)
            right_high = own_high[:, columns]
            right_low = own_low[:, columns]
            total = total + contract(high, right_high) + contract(high, right_low) + contract(low, right_high)
    own_diag[...] = total
    for step in range(1, 8):
        other = lax.rem(row + step, 8)
        piece = pl.ds(pl.multiple_of(other * 32, 32), 32)
        send(own_diag.at[piece, :], got_diag.at[row], send5.at[step], recv5.at[row], (other, col))
    for copy in sent[:-7]:
        copy.wait_send()
    here = pl.ds(pl.multiple_of(row * 32, 32), 32)
    result = diag_inv[0, here, :] + own_diag[here, :]
    for step in range(1, 8):
        other = lax.rem(row + step, 8)
        wait_recv(got_diag.at[other], send5.at[step], recv5.at[other])
        result = result + got_diag[other]
    sum_diag[...] = result
    for step in range(1, 8):
        other = lax.rem(row + step, 8)
        send(sum_diag, all_diag.at[row], send6.at[step], recv6.at[row], (other, col))
    diag_out[0, here, :] = result
    for item in range(ITEMS):
        for unit in range(2):
            send_piece(item, ITEM_DX[item], item < EVENTS, ITEM_PLACE[item], unit, False)
    for step in range(1, 8):
        other = lax.rem(row + step, 8)
        wait_recv(all_diag.at[other], send6.at[step], recv6.at[other])
        diag_out[0, pl.ds(pl.multiple_of(other * 32, 32), 32), :] = all_diag[other]

    for copy in sent[-14:]:
        copy.wait_send()


def local(panel_t, ancestor, structure, diag_inv):
    vmem = pltpu.VMEM
    dma = pltpu.SemaphoreType.DMA
    product, diag = pl.pallas_call(
        kernel,
        out_shape=(
            vmem((256, 1024), F32),
            vmem((1, 256, 256), F32),
        ),
        in_specs=[
            pl.BlockSpec(memory_space=pl.ANY),
            pl.BlockSpec(memory_space=pl.ANY),
            pl.BlockSpec(memory_space=pltpu.SMEM),
            pl.BlockSpec(memory_space=pl.ANY),
        ],
        out_specs=(pl.BlockSpec(memory_space=vmem), pl.BlockSpec(memory_space=vmem)),
        scratch_shapes=[
            vmem((1, 256, 1024), F32),
            vmem((1024, 512), F32),
            vmem((1, 256, 256), F32),
            vmem((2, EVENTS, 64, 1024), F32),
            vmem((2, 1024, 256), F32),
            vmem((4, 1024, 256), BF16),
            vmem((4, 1024, 256), BF16),
            vmem((EVENTS, 128, 1024), BF16),
            vmem((EVENTS, 128, 1024), BF16),
            vmem((256, 1024), BF16),
            vmem((256, 1024), BF16),
            vmem((ITEMS, NY, 2, 32, 256), F32),
            vmem((ITEMS, 2, 32, 256), F32),
            vmem((ITEMS, 2, 2, 32, 256), F32),
            vmem((ITEMS, 2, 2, 2, 8, 256), F32),
            vmem((ITEMS, 2, 2, 8, 256), F32),
            vmem((ITEMS, 2, 2, 8, 256), F32),
            vmem((2, 2, 4, 64, 256), F32),
            vmem((256, 256), F32),
            vmem((8, 32, 256), F32),
            vmem((32, 256), F32),
            vmem((8, 32, 256), F32),
            dma((12,)),
            dma((EVENTS,)),
            dma((EVENTS,)),
            dma((EVENTS,)),
            dma((2,)),
            dma((2,)),
            dma((ITEMS, 2)),
            dma((ITEMS, 2)),
            dma((ITEMS, 2)),
            dma((ITEMS, 2)),
            dma((ITEMS,)),
            dma((ITEMS,)),
            dma((ITEMS, 2)),
            dma((2, 4, 8)),
            dma((8,)),
            dma((8,)),
            dma((8,)),
            dma((8,)),
            dma((3,)),
        ],
        compiler_params=pltpu.CompilerParams(
            collective_id=0, has_side_effects=True, vmem_limit_bytes=60 * 1024 * 1024
        ),
        name="level_update",
    )(panel_t, ancestor, structure, diag_inv)
    return -product, diag


def solution(mesh):
    return jax.shard_map(
        local,
        mesh=mesh,
        in_specs=(P("pcol", None, "prow"), P("prow", "pcol"), P(), P("pcol", None, None)),
        out_specs=(P("pcol", "prow"), P("pcol", None, None)),
        check_vma=False,
    )
```

```python
import functools

import jax
import jax.numpy as jnp
from jax import lax
from jax.experimental import pallas as pl
from jax.experimental.pallas import tpu as pltpu
from jax.sharding import PartitionSpec as P

MESH = pl.DeviceIdType.MESH
F32 = jnp.float32
BF16 = jnp.bfloat16

DX = (0, 0, 0, 0, -1, -1, 1, 1, -1, -1, 1, 1, 2, 2, 2, 2)
QUARTER = (0, 1, 2, 3, 0, 1, 3, 2, 2, 3, 1, 0, 0, 1, 3, 2)
EVENTS = 16
TO_RIGHT = {0: 4, 1: 5, 2: 8, 3: 9, 4: 12, 5: 13}
TO_LEFT = {3: 6, 2: 7, 1: 10, 0: 11, 6: 14, 7: 15}
PAIRS = ((0, 1), (2, 3), (4, 5), (7, 6), (8, 9), (11, 10), (12, 13), (15, 14))
ITEMS = 32
ORDER = (
    "M0 M1 M2 M3", "A0 B0 A1 B1", "F4 F6 A2 B2", "A3 B3 M4 M6", "C0 C1 F5 F7", "C2 C3 M5 A4",
    "A6 B4 B6 M7", "F8 F10 A5 B5", "C4 M8 M10 A7", "B7 C6 C5 F9", "F11 A8 B8 G2", "M16 A10 B10 M9",
    "M11 M17 A16 B16", "M18 F12 F14 M19", "A9 B9 A11 B11", "M20 A17 B17 M12", "M14 A18 F13 F15", "A19 B18 B19 M21",
    "C7 C8 M13 M15", "A20 B20 M22 M23", "A12 A14 B12 B14", "C9 C10 C11 C16", "C17 C18 C19 A21", "B21 A13 B13 A15",
    "B15 G3 M24 M25", "A22 A23 B22 B23", "M26 M27 M28 M29", "M30 M31 D0 D1", "D2 D3 D4 D5", "D6 D7 D8 D9",
    "D10 D11 C12 D16", "A24 B24 C13 D17", "C14 A25 B25 C15", "D18 C20 C21 D19", "C22 C23 A26 B26", "A27 B27 A28 B28",
    "A29 B29 D12 A30", "B30 A31 B31 D13", "D14 D15 D20 D21", "D22 D23 C24 C25", "D24 C26 C27 D25", "C28 D26 C29 D27",
    "C30 D28 C31 D29", "D30 D31",
)
NX, NY = 4, 4


def parts(item):
    if item < EVENTS:
        return ((item, 0), (item, 1))
    first, second = PAIRS[(item - EVENTS) % 8]
    block = 2 + (item - EVENTS) // 8
    return ((first, block), (second, block))


def split(value):
    high = value.astype(BF16)
    low = (value - high.astype(F32)).astype(BF16)
    return high, low


def pick(table, index):
    value = jnp.int32(table[0])
    for place in range(1, len(table)):
        value = jnp.where(index == place, jnp.int32(table[place]), value)
    return value


def kernel(
    panel_hbm, ancestor_hbm, structure, diag_hbm, panel_out, diag_out,
    panel, ancestor, diag_inv, gathered, b_pair, b_high, b_low, a_high, a_low, own_high, own_low, partial, got1, got2, owned, got3, final, arrived, own_diag, got_diag,
    sum_diag, all_diag,
    gather_send, gather_recv, core_send, core_recv, pair_send, pair_recv, send1, recv1, send2, recv2, send3, recv3, send4, recv4,
    send5, recv5, send6, recv6, load_sem,
):
    row = lax.axis_index("prow")
    col = lax.axis_index("pcol")
    core = lax.rem(col, 2)
    zl = lax.rem(col // 2, 2)
    x = col // 4
    y = lax.rem(row, NY)
    zh = row // NY

    def at_col(xx, zz, cc):
        return (xx * 2 + zz) * 2 + cc

    right = (row, at_col(lax.rem(x + 1, NX), zl, core))
    left = (row, at_col(lax.rem(x + NX - 1, NX), zl, core))
    z_pair = (row, at_col(x, 1 - zl, core))
    twin = (row, at_col(x, zl, 1 - core))
    y_up, y_down, y_far = lax.rem(y + 1, NY), lax.rem(y + NY - 1, NY), lax.rem(y + 2, NY)
    up = (zh * NY + y_up, col)
    down = (zh * NY + y_down, col)
    z_far = ((1 - zh) * NY + y, col)
    home_rows = (x * 2 + zl, x * 2 + 1 - zl)

    barrier = pltpu.get_barrier_semaphore()

    def greet(device):
        pl.semaphore_signal(barrier, inc=1, device_id=device, device_id_type=MESH)

    greeted = (right, left, z_pair, twin, up, down, z_far)
    for device in greeted:
        greet(device)

    copies = [
        pltpu.make_async_copy(panel_hbm, panel, load_sem.at[0]),
        pltpu.make_async_copy(ancestor_hbm, ancestor, load_sem.at[1]),
        pltpu.make_async_copy(diag_hbm, diag_inv, load_sem.at[2]),
    ]
    for copy in copies:
        copy.start()
    for copy in copies:
        copy.wait()

    def take_columns(block, value):
        high, low = split(value)
        b_high[block] = high
        b_low[block] = low

    for block in range(2):
        take_columns(block, ancestor[:, block * 256 : (block + 1) * 256])

    def home_node(dx, unit):
        return at_col(lax.rem(x + NX + dx, NX), zl, core if unit == 0 else 1 - core)

    def load(event, unit, value):
        node = home_node(DX[event], unit)
        for block in range(4):
            mask = structure[node, row * 4 + block].astype(F32)
            high, low = split(value[:, block * 256 : (block + 1) * 256] * mask)
            a_high[event, unit * 64 : (unit + 1) * 64, block * 256 : (block + 1) * 256] = high
            a_low[event, unit * 64 : (unit + 1) * 64, block * 256 : (block + 1) * 256] = low

    for event in range(4):
        load(event, 0, panel[0, event * 64 : (event + 1) * 64, :])

    pl.semaphore_wait(barrier, len(greeted))

    sent = []

    def send(source, target, send_sem, recv_sem, device):
        copy = pltpu.make_async_remote_copy(
            src_ref=source, dst_ref=target, send_sem=send_sem, recv_sem=recv_sem, device_id=device, device_id_type=MESH
        )
        copy.start()
        sent.append(copy)

    def wait_recv(target, send_sem, recv_sem):
        pltpu.make_async_remote_copy(
            src_ref=target, dst_ref=target, send_sem=send_sem, recv_sem=recv_sem, device_id=twin, device_id_type=MESH
        ).wait_recv()

    def mine(event):
        if event < 4:
            return panel.at[0, pl.ds(event * 64, 64), :]
        return gathered.at[0, event]

    count = [0]

    def pass_on(event, table, device):
        if event in table:
            there = table[event]
            send(mine(event), gathered.at[0, there], gather_send.at[count[0]], gather_recv.at[there], device)
            count[0] += 1

    def to_twin(event):
        send(mine(event), gathered.at[1, event], core_send.at[event], core_recv.at[event], twin)

    def arrive(event):
        wait_recv(gathered.at[0, event], gather_send.at[0], gather_recv.at[event])
        pass_on(event, TO_RIGHT, right)
        pass_on(event, TO_LEFT, left)
        to_twin(event)

    def take_pair(block):
        wait_recv(b_pair.at[block - 2], pair_send.at[block - 2], pair_recv.at[block - 2])
        take_columns(block, b_pair[block - 2])

    def multiply(item):
        if item < EVENTS:
            if item >= 4:
                load(item, 0, mine(item))
            wait_recv(gathered.at[1, item], core_send.at[0], core_recv.at[item])
            load(item, 1, gathered.at[1, item])
        (event0, block0), (event1, block1) = parts(item)

        @pl.loop(0, 2)
        def _(n):
            event = event0 + n * (event1 - event0)
            block = block0 + n * (block1 - block0)
            high = a_high[event]
            product = (
                jnp.dot(high, b_high[block], preferred_element_type=F32)
                + jnp.dot(high, b_low[block], preferred_element_type=F32)
                + jnp.dot(a_low[event], b_high[block], preferred_element_type=F32)
            )
            for unit in range(2):
                for yy in range(NY):
                    start = unit * 64 + yy * 16
                    partial[item, yy, n, unit * 16 : (unit + 1) * 16, :] = product[start : start + 16, :]

        send(partial.at[item, y_far, 0], got1.at[item, 0], send1.at[item, 0], recv1.at[item, 0], up)
        send(partial.at[item, y_far, 1], got1.at[item, 1], send1.at[item, 1], recv1.at[item, 1], down)

    def stage2(item, way):
        yy, device = ((y_up, up), (y_down, down))[way]
        wait_recv(got1.at[item, way], send1.at[item, way], recv1.at[item, way])
        partial[item, yy, way] += got1[item, way]
        send(partial.at[item, yy], got2.at[item, way], send2.at[item, way], recv2.at[item, way], device)

    def stage3(item):
        for way in range(2):
            wait_recv(got2.at[item, way], send2.at[item, way], recv2.at[item, way])
        for n in range(2):
            total = partial[item, y, n] + got2[item, 0, n] + got2[item, 1, n]
            for unit in range(2):
                for hz in range(2):
                    start = unit * 16 + hz * 8
                    owned[item, hz, unit, n] = total[start : start + 8, :]
        send(owned.at[item, 1 - zh], got3.at[item], send3.at[item], recv3.at[item], z_far)

    def stage4(item):
        wait_recv(got3.at[item], send3.at[item], recv3.at[item])
        final[item] = owned[item, zh] + got3[item]

    def send_piece(item, dx, own, place, unit, act):
        node = home_node(dx, unit)
        home_row = home_rows[0] if own else home_rows[1]
        here = jnp.logical_and(home_row == row, node == col)
        rows = pl.ds(pl.multiple_of(y * 16 + zh * 8, 8), 8)
        if own:
            target = arrived.at[core, :, place, rows, :]
        else:
            quarters = pl.ds(lax.rem(place, 2) * 2, 2)
            target = arrived.at[core, place // 2, quarters, rows, :]
        copy = pltpu.make_async_remote_copy(
            src_ref=final.at[item, unit], dst_ref=target, send_sem=send4.at[item, unit], recv_sem=recv4.at[core, place, row],
            device_id=(home_row, node), device_id_type=MESH,
        )
        if act:

            @pl.when(here)
            def _():
                if own:
                    arrived[core, :, place, rows, :] = final[item, unit]
                else:
                    arrived[core, place // 2, quarters, rows, :] = final[item, unit]

        @pl.when(jnp.logical_not(here))
        def _():
            if act:
                copy.start()
            else:
                copy.wait_send()

    ITEM_DX = DX + tuple(DX[parts(item)[0][0]] for item in range(EVENTS, ITEMS))
    ITEM_PLACE = QUARTER + tuple(
        (parts(item)[0][1] - 2) * 2 + QUARTER[parts(item)[0][0]] // 2 for item in range(EVENTS, ITEMS)
    )

    def spread(chips):
        order, lists = [], [list(items) for items in chips.values()]
        while any(lists):
            order += [items.pop(0) for items in lists if items]
        return tuple(order)

    def send_home(items, turn):
        item = pick(items, lax.rem(row + turn, len(items)))
        dx = pick(ITEM_DX, item)
        place = pick(ITEM_PLACE, item)
        for unit in range(2):

            @pl.when(item < EVENTS)
            def _():
                send_piece(item, dx, True, place, unit, True)

            @pl.when(item >= EVENTS)
            def _():
                send_piece(item, dx, False, place, unit, True)

    for turn in range(2):
        pass_on(turn, TO_RIGHT, right)
        pass_on(3 - turn, TO_LEFT, left)
    for block in range(2):
        send(ancestor.at[:, pl.ds(block * 256, 256)], b_pair.at[block], pair_send.at[block], pair_recv.at[block], z_pair)
    for event in range(4):
        to_twin(event)
    for turn in range(2, 4):
        pass_on(turn, TO_RIGHT, right)
        pass_on(3 - turn, TO_LEFT, left)
    work = {
        "F": arrive,
        "G": take_pair,
        "M": multiply,
        "A": lambda item: stage2(item, 0),
        "B": lambda item: stage2(item, 1),
        "C": stage3,
        "D": stage4,
    }
    for step in " ".join(ORDER).split():
        work[step[0]](int(step[1:]))
    chips = {}
    for item in range(ITEMS):
        chips.setdefault((ITEM_DX[item], item < EVENTS), []).append(item)
    turns = spread(chips)
    for turn in range(ITEMS):
        send_home(turns, turn)

    for block in range(4):
        mask = structure[col, row * 4 + block].astype(F32)
        high, low = split(panel[0, :, block * 256 : (block + 1) * 256] * mask)
        own_high[:, block * 256 : (block + 1) * 256] = high
        own_low[:, block * 256 : (block + 1) * 256] = low

    contract = functools.partial(
        lax.dot_general, dimension_numbers=(((1,), (1,)), ((), ())), preferred_element_type=F32
    )
    from_own = lax.rem(row, 2) == zl

    def take(side, place):
        for source in range(8):
            there = jnp.logical_and(source == row, at_col(row // 2, zl, side) == col)

            @pl.when(jnp.logical_not(there))
            def _():
                wait_recv(final.at[0, 0], send4.at[0, 0], recv4.at[side, place, source])

    total = jnp.zeros((256, 256), F32)
    for block in range(2):
        for side in range(2):
            for half in range(2):
                take_now = (block * 2 + half,)

                @pl.when(jnp.logical_not(from_own))
                def _():
                    take(side, take_now[0])

            if block == 0:

                @pl.when(from_own)
                def _():
                    for place in range(4):
                        take(side, place)

            columns = slice(side * 512 + block * 256, side * 512 + block * 256 + 256)
            value = arrived[side, block].reshape(256, 256)
            panel_out[:, columns] = value
            high, low = split(value)
            right_high = own_high[:, columns]
            right_low = own_low[:, columns]
            total = total + contract(high, right_high) + contract(high, right_low) + contract(low, right_high)
    own_diag[...] = total
    for step in range(1, 8):
        other = lax.rem(row + step, 8)
        piece = pl.ds(pl.multiple_of(other * 32, 32), 32)
        send(own_diag.at[piece, :], got_diag.at[row], send5.at[step], recv5.at[row], (other, col))
    for copy in sent[:-7]:
        copy.wait_send()
    here = pl.ds(pl.multiple_of(row * 32, 32), 32)
    result = diag_inv[0, here, :] + own_diag[here, :]
    for step in range(1, 8):
        other = lax.rem(row + step, 8)
        wait_recv(got_diag.at[other], send5.at[step], recv5.at[other])
        result = result + got_diag[other]
    sum_diag[...] = result
    for step in range(1, 8):
        other = lax.rem(row + step, 8)
        send(sum_diag, all_diag.at[row], send6.at[step], recv6.at[row], (other, col))
    diag_out[0, here, :] = result
    for item in range(ITEMS):
        for unit in range(2):
            send_piece(item, ITEM_DX[item], item < EVENTS, ITEM_PLACE[item], unit, False)
    for step in range(1, 8):
        other = lax.rem(row + step, 8)
        wait_recv(all_diag.at[other], send6.at[step], recv6.at[other])
        diag_out[0, pl.ds(pl.multiple_of(other * 32, 32), 32), :] = all_diag[other]

    for copy in sent[-14:]:
        copy.wait_send()


def local(panel_t, ancestor, structure, diag_inv):
    vmem = pltpu.VMEM
    dma = pltpu.SemaphoreType.DMA
    product, diag = pl.pallas_call(
        kernel,
        out_shape=(
            vmem((256, 1024), F32),
            vmem((1, 256, 256), F32),
        ),
        in_specs=[
            pl.BlockSpec(memory_space=pl.ANY),
            pl.BlockSpec(memory_space=pl.ANY),
            pl.BlockSpec(memory_space=pltpu.SMEM),
            pl.BlockSpec(memory_space=pl.ANY),
        ],
        out_specs=(pl.BlockSpec(memory_space=vmem), pl.BlockSpec(memory_space=vmem)),
        scratch_shapes=[
            vmem((1, 256, 1024), F32),
            vmem((1024, 512), F32),
            vmem((1, 256, 256), F32),
            vmem((2, EVENTS, 64, 1024), F32),
            vmem((2, 1024, 256), F32),
            vmem((4, 1024, 256), BF16),
            vmem((4, 1024, 256), BF16),
            vmem((EVENTS, 128, 1024), BF16),
            vmem((EVENTS, 128, 1024), BF16),
            vmem((256, 1024), BF16),
            vmem((256, 1024), BF16),
            vmem((ITEMS, NY, 2, 32, 256), F32),
            vmem((ITEMS, 2, 32, 256), F32),
            vmem((ITEMS, 2, 2, 32, 256), F32),
            vmem((ITEMS, 2, 2, 2, 8, 256), F32),
            vmem((ITEMS, 2, 2, 8, 256), F32),
            vmem((ITEMS, 2, 2, 8, 256), F32),
            vmem((2, 2, 4, 64, 256), F32),
            vmem((256, 256), F32),
            vmem((8, 32, 256), F32),
            vmem((32, 256), F32),
            vmem((8, 32, 256), F32),
            dma((12,)),
            dma((EVENTS,)),
            dma((EVENTS,)),
            dma((EVENTS,)),
            dma((2,)),
            dma((2,)),
            dma((ITEMS, 2)),
            dma((ITEMS, 2)),
            dma((ITEMS, 2)),
            dma((ITEMS, 2)),
            dma((ITEMS,)),
            dma((ITEMS,)),
            dma((ITEMS, 2)),
            dma((2, 4, 8)),
            dma((8,)),
            dma((8,)),
            dma((8,)),
            dma((8,)),
            dma((3,)),
        ],
        compiler_params=pltpu.CompilerParams(
            collective_id=0, has_side_effects=True, vmem_limit_bytes=60 * 1024 * 1024
        ),
        name="level_update",
    )(panel_t, ancestor, structure, diag_inv)
    return -product, diag


def solution(mesh):
    return jax.shard_map(
        local,
        mesh=mesh,
        in_specs=(P("pcol", None, "prow"), P("prow", "pcol"), P(), P("pcol", None, None)),
        out_specs=(P("pcol", "prow"), P("pcol", None, None)),
        check_vma=False,
    )
```

```python
import functools

import jax
import jax.numpy as jnp
from jax import lax
from jax.experimental import pallas as pl
from jax.experimental.pallas import tpu as pltpu
from jax.sharding import PartitionSpec as P

MESH = pl.DeviceIdType.MESH
F32 = jnp.float32
BF16 = jnp.bfloat16

DX = (0, 0, 0, 0, -1, -1, 1, 1, -1, -1, 1, 1, 2, 2, 2, 2)
QUARTER = (0, 1, 2, 3, 0, 1, 3, 2, 2, 3, 1, 0, 0, 1, 3, 2)
EVENTS = 16
TO_RIGHT = {0: 4, 1: 5, 2: 8, 3: 9, 4: 12, 5: 13}
TO_LEFT = {3: 6, 2: 7, 1: 10, 0: 11, 6: 14, 7: 15}
PAIRS = ((0, 1), (2, 3), (4, 5), (7, 6), (8, 9), (11, 10), (12, 13), (15, 14))
ITEMS = 32
ORDER = (
    "M0 M1 M2 M3", "A0 B0 A1 B1", "F4 F6 A2 B2", "A3 B3 M4 M6", "C0 C1 F5 F7", "C2 C3 M5 A4",
    "A6 B4 B6 M7", "F8 F10 A5 B5", "M8 M10 C4 C6", "A7 B7 F9 F11", "G2 M16 A8 B8", "M17 A10 B10 M9",
    "M11 A16 B16 M18", "F12 F14 M19 A17", "B17 M20 M12 A9", "B9 M14 A11 B11", "F13 F15 M21 C5", "A18 B18 C7 C8",
    "A19 B19 C10 M13", "M15 A12 A20 B12", "B20 M22 M23 A14", "B14 C9 C16 C17", "C11 A21 B21 C18", "G3 M24 A13 A15",
    "B13 B15 M25 M26", "M27 M28 A22 B22", "A23 B23 M29 M30", "M31 C12 C14 C19", "A24 B24 C20 C21", "D0 D1 D2 D3",
    "D4 D5 C13 D6", "D7 D8 D9 D10", "D11 D16 D17 D18", "C15 A25 B25 D12", "A26 B26 D14 A27", "B27 D19 A28 B28",
    "D20 D21 C22 D13", "D15 C23 A29 B29", "A30 B30 A31 B31", "D22 C24 D23 C25", "C26 C27 D24 C28", "D25 C29 D26 C30",
    "D27 C31 D28 D29", "D30 D31",
)
NX, NY = 4, 4


def parts(item):
    if item < EVENTS:
        return ((item, 0), (item, 1))
    first, second = PAIRS[(item - EVENTS) % 8]
    block = 2 + (item - EVENTS) // 8
    return ((first, block), (second, block))


def split(value):
    high = value.astype(BF16)
    low = (value - high.astype(F32)).astype(BF16)
    return high, low


def pick(table, index):
    value = jnp.int32(table[0])
    for place in range(1, len(table)):
        value = jnp.where(index == place, jnp.int32(table[place]), value)
    return value


def kernel(
    panel_hbm, ancestor_hbm, structure, diag_hbm, panel_out, diag_out,
    panel, ancestor, diag_inv, gathered, b_pair, b_high, b_low, a_high, a_low, own_high, own_low, partial, got1, got2, owned, got3, final, arrived, own_diag, got_diag,
    sum_diag, all_diag,
    gather_send, gather_recv, core_send, core_recv, pair_send, pair_recv, send1, recv1, send2, recv2, send3, recv3, send4, recv4,
    send5, recv5, send6, recv6, load_sem,
):
    row = lax.axis_index("prow")
    col = lax.axis_index("pcol")
    core = lax.rem(col, 2)
    zl = lax.rem(col // 2, 2)
    x = col // 4
    y = lax.rem(row, NY)
    zh = row // NY

    def at_col(xx, zz, cc):
        return (xx * 2 + zz) * 2 + cc

    right = (row, at_col(lax.rem(x + 1, NX), zl, core))
    left = (row, at_col(lax.rem(x + NX - 1, NX), zl, core))
    z_pair = (row, at_col(x, 1 - zl, core))
    twin = (row, at_col(x, zl, 1 - core))
    y_up, y_down, y_far = lax.rem(y + 1, NY), lax.rem(y + NY - 1, NY), lax.rem(y + 2, NY)
    up = (zh * NY + y_up, col)
    down = (zh * NY + y_down, col)
    z_far = ((1 - zh) * NY + y, col)
    home_rows = (x * 2 + zl, x * 2 + 1 - zl)

    barrier = pltpu.get_barrier_semaphore()

    def greet(device):
        pl.semaphore_signal(barrier, inc=1, device_id=device, device_id_type=MESH)

    greeted = (right, left, z_pair, twin, up, down, z_far)
    for device in greeted:
        greet(device)

    copies = [
        pltpu.make_async_copy(panel_hbm, panel, load_sem.at[0]),
        pltpu.make_async_copy(ancestor_hbm, ancestor, load_sem.at[1]),
        pltpu.make_async_copy(diag_hbm, diag_inv, load_sem.at[2]),
    ]
    for copy in copies:
        copy.start()
    for copy in copies:
        copy.wait()

    def take_columns(block, value):
        high, low = split(value)
        b_high[block] = high
        b_low[block] = low

    for block in range(2):
        take_columns(block, ancestor[:, block * 256 : (block + 1) * 256])

    def home_node(dx, unit):
        return at_col(lax.rem(x + NX + dx, NX), zl, core if unit == 0 else 1 - core)

    def load(event, unit, value):
        node = home_node(DX[event], unit)
        for block in range(4):
            mask = structure[node, row * 4 + block].astype(F32)
            high, low = split(value[:, block * 256 : (block + 1) * 256] * mask)
            a_high[event, unit * 64 : (unit + 1) * 64, block * 256 : (block + 1) * 256] = high
            a_low[event, unit * 64 : (unit + 1) * 64, block * 256 : (block + 1) * 256] = low

    for event in range(4):
        load(event, 0, panel[0, event * 64 : (event + 1) * 64, :])

    pl.semaphore_wait(barrier, len(greeted))

    sent = []

    def send(source, target, send_sem, recv_sem, device):
        copy = pltpu.make_async_remote_copy(
            src_ref=source, dst_ref=target, send_sem=send_sem, recv_sem=recv_sem, device_id=device, device_id_type=MESH
        )
        copy.start()
        sent.append(copy)

    def wait_recv(target, send_sem, recv_sem):
        pltpu.make_async_remote_copy(
            src_ref=target, dst_ref=target, send_sem=send_sem, recv_sem=recv_sem, device_id=twin, device_id_type=MESH
        ).wait_recv()

    def mine(event):
        if event < 4:
            return panel.at[0, pl.ds(event * 64, 64), :]
        return gathered.at[0, event]

    count = [0]

    def pass_on(event, table, device):
        if event in table:
            there = table[event]
            send(mine(event), gathered.at[0, there], gather_send.at[count[0]], gather_recv.at[there], device)
            count[0] += 1

    def to_twin(event):
        send(mine(event), gathered.at[1, event], core_send.at[event], core_recv.at[event], twin)

    def arrive(event):
        wait_recv(gathered.at[0, event], gather_send.at[0], gather_recv.at[event])
        pass_on(event, TO_RIGHT, right)
        pass_on(event, TO_LEFT, left)
        to_twin(event)

    def take_pair(block):
        wait_recv(b_pair.at[block - 2], pair_send.at[block - 2], pair_recv.at[block - 2])
        take_columns(block, b_pair[block - 2])

    def multiply(item):
        if item < EVENTS:
            if item >= 4:
                load(item, 0, mine(item))
            wait_recv(gathered.at[1, item], core_send.at[0], core_recv.at[item])
            load(item, 1, gathered.at[1, item])
        (event0, block0), (event1, block1) = parts(item)

        @pl.loop(0, 2)
        def _(n):
            event = event0 + n * (event1 - event0)
            block = block0 + n * (block1 - block0)
            high = a_high[event]
            product = (
                jnp.dot(high, b_high[block], preferred_element_type=F32)
                + jnp.dot(high, b_low[block], preferred_element_type=F32)
                + jnp.dot(a_low[event], b_high[block], preferred_element_type=F32)
            )
            for unit in range(2):
                for yy in range(NY):
                    start = unit * 64 + yy * 16
                    partial[item, yy, n, unit * 16 : (unit + 1) * 16, :] = product[start : start + 16, :]

        send(partial.at[item, y_far, 0], got1.at[item, 0], send1.at[item, 0], recv1.at[item, 0], up)
        send(partial.at[item, y_far, 1], got1.at[item, 1], send1.at[item, 1], recv1.at[item, 1], down)

    def stage2(item, way):
        yy, device = ((y_up, up), (y_down, down))[way]
        wait_recv(got1.at[item, way], send1.at[item, way], recv1.at[item, way])
        partial[item, yy, way] += got1[item, way]
        send(partial.at[item, yy], got2.at[item, way], send2.at[item, way], recv2.at[item, way], device)

    def stage3(item):
        for way in range(2):
            wait_recv(got2.at[item, way], send2.at[item, way], recv2.at[item, way])
        for n in range(2):
            total = partial[item, y, n] + got2[item, 0, n] + got2[item, 1, n]
            for unit in range(2):
                for hz in range(2):
                    start = unit * 16 + hz * 8
                    owned[item, hz, unit, n] = total[start : start + 8, :]
        send(owned.at[item, 1 - zh], got3.at[item], send3.at[item], recv3.at[item], z_far)

    def stage4(item):
        wait_recv(got3.at[item], send3.at[item], recv3.at[item])
        final[item] = owned[item, zh] + got3[item]

    def send_piece(item, dx, own, place, unit, act):
        node = home_node(dx, unit)
        home_row = home_rows[0] if own else home_rows[1]
        here = jnp.logical_and(home_row == row, node == col)
        rows = pl.ds(pl.multiple_of(y * 16 + zh * 8, 8), 8)
        if own:
            target = arrived.at[core, :, place, rows, :]
        else:
            quarters = pl.ds(lax.rem(place, 2) * 2, 2)
            target = arrived.at[core, place // 2, quarters, rows, :]
        copy = pltpu.make_async_remote_copy(
            src_ref=final.at[item, unit], dst_ref=target, send_sem=send4.at[item, unit], recv_sem=recv4.at[core, place, row],
            device_id=(home_row, node), device_id_type=MESH,
        )
        if act:

            @pl.when(here)
            def _():
                if own:
                    arrived[core, :, place, rows, :] = final[item, unit]
                else:
                    arrived[core, place // 2, quarters, rows, :] = final[item, unit]

        @pl.when(jnp.logical_not(here))
        def _():
            if act:
                copy.start()
            else:
                copy.wait_send()

    ITEM_DX = DX + tuple(DX[parts(item)[0][0]] for item in range(EVENTS, ITEMS))
    ITEM_PLACE = QUARTER + tuple(
        (parts(item)[0][1] - 2) * 2 + QUARTER[parts(item)[0][0]] // 2 for item in range(EVENTS, ITEMS)
    )

    def spread(chips):
        order, lists = [], [list(items) for items in chips.values()]
        while any(lists):
            order += [items.pop(0) for items in lists if items]
        return tuple(order)

    def send_home(items, turn):
        item = pick(items, lax.rem(row + turn, len(items)))
        dx = pick(ITEM_DX, item)
        place = pick(ITEM_PLACE, item)
        for unit in range(2):

            @pl.when(item < EVENTS)
            def _():
                send_piece(item, dx, True, place, unit, True)

            @pl.when(item >= EVENTS)
            def _():
                send_piece(item, dx, False, place, unit, True)

    for turn in range(2):
        pass_on(turn, TO_RIGHT, right)
        pass_on(3 - turn, TO_LEFT, left)
    for block in range(2):
        send(ancestor.at[:, pl.ds(block * 256, 256)], b_pair.at[block], pair_send.at[block], pair_recv.at[block], z_pair)
    for event in range(4):
        to_twin(event)
    for turn in range(2, 4):
        pass_on(turn, TO_RIGHT, right)
        pass_on(3 - turn, TO_LEFT, left)
    work = {
        "F": arrive,
        "G": take_pair,
        "M": multiply,
        "A": lambda item: stage2(item, 0),
        "B": lambda item: stage2(item, 1),
        "C": stage3,
        "D": stage4,
    }
    for step in " ".join(ORDER).split():
        work[step[0]](int(step[1:]))
    chips = {}
    for item in range(ITEMS):
        chips.setdefault((ITEM_DX[item], item < EVENTS), []).append(item)
    turns = spread(chips)
    for turn in range(ITEMS):
        send_home(turns, turn)

    for block in range(4):
        mask = structure[col, row * 4 + block].astype(F32)
        high, low = split(panel[0, :, block * 256 : (block + 1) * 256] * mask)
        own_high[:, block * 256 : (block + 1) * 256] = high
        own_low[:, block * 256 : (block + 1) * 256] = low

    contract = functools.partial(
        lax.dot_general, dimension_numbers=(((1,), (1,)), ((), ())), preferred_element_type=F32
    )
    from_own = lax.rem(row, 2) == zl

    def take(side, place):
        for source in range(8):
            there = jnp.logical_and(source == row, at_col(row // 2, zl, side) == col)

            @pl.when(jnp.logical_not(there))
            def _():
                wait_recv(final.at[0, 0], send4.at[0, 0], recv4.at[side, place, source])

    total = jnp.zeros((256, 256), F32)
    for block in range(2):
        for side in range(2):
            for half in range(2):
                take_now = (block * 2 + half,)

                @pl.when(jnp.logical_not(from_own))
                def _():
                    take(side, take_now[0])

            if block == 0:

                @pl.when(from_own)
                def _():
                    for place in range(4):
                        take(side, place)

            columns = slice(side * 512 + block * 256, side * 512 + block * 256 + 256)
            value = arrived[side, block].reshape(256, 256)
            panel_out[:, columns] = value
            high, low = split(value)
            right_high = own_high[:, columns]
            right_low = own_low[:, columns]
            total = total + contract(high, right_high) + contract(high, right_low) + contract(low, right_high)
    own_diag[...] = total
    for step in range(1, 8):
        other = lax.rem(row + step, 8)
        piece = pl.ds(pl.multiple_of(other * 32, 32), 32)
        send(own_diag.at[piece, :], got_diag.at[row], send5.at[step], recv5.at[row], (other, col))
    for copy in sent[:-7]:
        copy.wait_send()
    here = pl.ds(pl.multiple_of(row * 32, 32), 32)
    result = diag_inv[0, here, :] + own_diag[here, :]
    for step in range(1, 8):
        other = lax.rem(row + step, 8)
        wait_recv(got_diag.at[other], send5.at[step], recv5.at[other])
        result = result + got_diag[other]
    sum_diag[...] = result
    for step in range(1, 8):
        other = lax.rem(row + step, 8)
        send(sum_diag, all_diag.at[row], send6.at[step], recv6.at[row], (other, col))
    diag_out[0, here, :] = result
    for item in range(ITEMS):
        for unit in range(2):
            send_piece(item, ITEM_DX[item], item < EVENTS, ITEM_PLACE[item], unit, False)
    for step in range(1, 8):
        other = lax.rem(row + step, 8)
        wait_recv(all_diag.at[other], send6.at[step], recv6.at[other])
        diag_out[0, pl.ds(pl.multiple_of(other * 32, 32), 32), :] = all_diag[other]

    for copy in sent[-14:]:
        copy.wait_send()


def local(panel_t, ancestor, structure, diag_inv):
    vmem = pltpu.VMEM
    dma = pltpu.SemaphoreType.DMA
    product, diag = pl.pallas_call(
        kernel,
        out_shape=(
            vmem((256, 1024), F32),
            vmem((1, 256, 256), F32),
        ),
        in_specs=[
            pl.BlockSpec(memory_space=pl.ANY),
            pl.BlockSpec(memory_space=pl.ANY),
            pl.BlockSpec(memory_space=pltpu.SMEM),
            pl.BlockSpec(memory_space=pl.ANY),
        ],
        out_specs=(pl.BlockSpec(memory_space=vmem), pl.BlockSpec(memory_space=vmem)),
        scratch_shapes=[
            vmem((1, 256, 1024), F32),
            vmem((1024, 512), F32),
            vmem((1, 256, 256), F32),
            vmem((2, EVENTS, 64, 1024), F32),
            vmem((2, 1024, 256), F32),
            vmem((4, 1024, 256), BF16),
            vmem((4, 1024, 256), BF16),
            vmem((EVENTS, 128, 1024), BF16),
            vmem((EVENTS, 128, 1024), BF16),
            vmem((256, 1024), BF16),
            vmem((256, 1024), BF16),
            vmem((ITEMS, NY, 2, 32, 256), F32),
            vmem((ITEMS, 2, 32, 256), F32),
            vmem((ITEMS, 2, 2, 32, 256), F32),
            vmem((ITEMS, 2, 2, 2, 8, 256), F32),
            vmem((ITEMS, 2, 2, 8, 256), F32),
            vmem((ITEMS, 2, 2, 8, 256), F32),
            vmem((2, 2, 4, 64, 256), F32),
            vmem((256, 256), F32),
            vmem((8, 32, 256), F32),
            vmem((32, 256), F32),
            vmem((8, 32, 256), F32),
            dma((12,)),
            dma((EVENTS,)),
            dma((EVENTS,)),
            dma((EVENTS,)),
            dma((2,)),
            dma((2,)),
            dma((ITEMS, 2)),
            dma((ITEMS, 2)),
            dma((ITEMS, 2)),
            dma((ITEMS, 2)),
            dma((ITEMS,)),
            dma((ITEMS,)),
            dma((ITEMS, 2)),
            dma((2, 4, 8)),
            dma((8,)),
            dma((8,)),
            dma((8,)),
            dma((8,)),
            dma((3,)),
        ],
        compiler_params=pltpu.CompilerParams(
            collective_id=0, has_side_effects=True, vmem_limit_bytes=60 * 1024 * 1024
        ),
        name="level_update",
    )(panel_t, ancestor, structure, diag_inv)
    return -product, diag


def solution(mesh):
    return jax.shard_map(
        local,
        mesh=mesh,
        in_specs=(P("pcol", None, "prow"), P("prow", "pcol"), P(), P("pcol", None, None)),
        out_specs=(P("pcol", "prow"), P("pcol", None, None)),
        check_vma=False,
    )
```
